32 devices in a mesh: groups: 2 (over x), expert: 8 (over z, y), mp: 2 (over core).
Axes of the slice: x: 2, y: 2, z: 4, core: 2. Of those that a mesh axis runs over, the one named last changes fastest.
Arguments:
- residual: bfloat16 [512, 5120], P(('groups', 'expert'), 'mp'), parts along dimension 0, may hold values from -6 to 6
- norm_gain: bfloat16 [5120], P('mp'), may hold values from 0.099609375 to 1.8984375
- router_weight: bfloat16 [640, 128], replicated, may hold values from -0.25 to 0.25
- expert_ids: int32 [512, 8, 2], P(('groups', 'expert')), parts along dimension 0, may hold values from 0 to 127, all different within a row; in each aligned block of 256 rows (0 to 255, 256 to 511, ..., all dimensions but the last counted through in order) at most 5 rows name the same one
- expert_in: bfloat16 [128, 640, 1280], P('expert', None, 'mp'), may hold values from -0.25 to 0.25
- expert_out: bfloat16 [128, 1280, 640], P('expert', 'mp'), may hold values from -0.15625 to 0.15625
- queries: bfloat16 [512, 5120], P(('groups', 'expert'), 'mp'), parts along dimension 0, may hold values from -6 to 6
- new_keys: bfloat16 [512, 1024], P(('groups', 'expert'), 'mp'), parts along dimension 0, may hold values from -6 to 6
- new_values: bfloat16 [512, 1024], P(('groups', 'expert'), 'mp'), parts along dimension 0, may hold values from -6 to 6
- cache_keys: bfloat16 [512, 128, 1024], P(('groups', 'expert'), None, 'mp'), parts along dimension 0, may hold values from -6 to 6
- cache_values: bfloat16 [512, 128, 1024], P(('groups', 'expert'), None, 'mp'), parts along dimension 0, may hold values from -6 to 6
- lengths: int32 [512], P(('groups', 'expert')), parts along dimension 0, may hold values from 1 to 128
Outputs:
- attention: bfloat16 [512, 5120], P(('groups', 'expert'), 'mp'), parts along dimension 0
- mixed: bfloat16 [512, 5120], P(('groups', 'expert'), 'mp'), parts along dimension 0
The draws below stay inside these ranges and needn't reach their ends.
There are 2 independent parts, one for each index of `groups`. The reference program is written for one: setup_inputs(seed, part) draws one part's arguments, and reference() takes and returns one part's arrays. A program takes and returns all parts, laid end to end along the dimension named above; an argument that names none is the same for every part. Nothing has to cross between parts.
Inputs may be any that keep to these rules, and one draw needn't show every extreme that they name: `expert_ids`: within the 8 sub-tokens of each aligned block of 32 tokens, no expert is named more than 5 times, a bound that some block reaches; the 2 experts of one sub-token differ.
All inputs are finite; a program needn't handle non-finite values.
Results may differ from the reference program's by a relative error of at most 0.006.
Values may be sent and summed in bfloat16 or wider, within the bound.
No kernel may reach another device: no remote copies, remote signals or barrier semaphores. Data moves between devices by JAX's collectives and lax.ppermute only.
A program may use at most 128 MiB of HBM per device.

```python
import math
import jax
import jax.numpy as jnp
import numpy as np
from jax import lax

D = 5120
SUB = 8
HEADS = 40
HD = 128
KV_HEADS = 8
EFF = 1280
EXPERTS = 128
TOP = 2
CAP = 5
CACHE = 128
TOK_DEV = 32
TOKENS = 256
N_EXPERT = 8


def drawn_draw(key):
    base_key = jax.random.fold_in(key, 7001)
    subkeys = jax.random.split(base_key, 3)
    per_group = HEADS // KV_HEADS
    query_part = jnp.clip(jax.random.normal(subkeys[0], (TOKENS, KV_HEADS, per_group, HD), jnp.float32), -6.0, 6.0)
    cache_part = jnp.clip(jax.random.normal(subkeys[1], (TOKENS, CACHE, KV_HEADS, HD), jnp.float32), -6.0, 6.0)
    fresh_part = jnp.clip(jax.random.normal(subkeys[2], (TOKENS, KV_HEADS, HD), jnp.float32), -6.0, 6.0)
    return (query_part, cache_part, fresh_part)


def draw_queries(key, part):
    query_part, cache_part, fresh_part = drawn_draw(key)
    return query_part.reshape(TOKENS, HEADS * HD).astype(jnp.bfloat16)


def draw_cache_keys(key, part):
    query_part, cache_part, fresh_part = drawn_draw(key)
    return cache_part.reshape(TOKENS, CACHE, KV_HEADS * HD).astype(jnp.bfloat16)


def draw_new_keys(key, part):
    query_part, cache_part, fresh_part = drawn_draw(key)
    return fresh_part.reshape(TOKENS, KV_HEADS * HD).astype(jnp.bfloat16)


def with_ends(result, stream_key, low, high):
    shape = result.shape
    place = [jax.random.randint(jax.random.fold_in(stream_key, axis), (), 0, shape[axis]) for axis in range(len(shape))]
    result = result.at[tuple(place)].set(low)
    longest = shape.index(max(shape))
    place[longest] = (place[longest] + 1) % shape[longest]
    return result.at[tuple(place)].set(high)


def shard_levels(key, dims, cuts, least, top_value):
    level = 1.0
    for position, shards_of in cuts:
        heights = jax.random.uniform(jax.random.fold_in(jax.random.fold_in(key, 6), position), (shards_of,), jnp.float32, least / len(cuts), top_value / len(cuts))
        level = level * jnp.repeat(jnp.exp(heights), dims[position] // shards_of).reshape((-1,) + (1,) * (len(dims) - 1 - position))
    return level


def assign_block(rng, own, number, rows, count, top, limit, slope):
    ranking = jax.random.permutation(rng, count)
    heavy_load, common = load_shares(count, rows * top, limit, slope, True), load_shares(count, rows * top, limit, slope, False)
    places = jnp.arange(count)

    def named(sizes, rotation):
        used = int((sizes > 0).sum())
        fixed = max(1, used // 4)
        shifted = fixed + (places - fixed + rotation * (used - fixed)) % max(1, count - fixed)
        return jnp.zeros((count,), jnp.int32).at[ranking[jnp.where(places < fixed, places, shifted)]].set(jnp.asarray(sizes, jnp.int32))

    sizes = jnp.where(number % 4 == 0, named(heavy_load, number // 4), named(common, number - number // 4 - 1))
    mixed = jax.random.permutation(jax.random.fold_in(own, 3), count)
    giver, sink = mixed[0:count // 2 * 2:2], mixed[1:count // 2 * 2:2]
    room = jnp.minimum(sizes[giver] - 1, limit - sizes[sink]) // 2
    room = jnp.where((giver == ranking[0]) | (sink == ranking[0]) | (sizes[sink] == 0), 0, jnp.maximum(room, 0))
    shifted = jax.random.randint(jax.random.fold_in(own, 4), (count // 2,), 0, 1 << 20) % (room + 1)
    sizes = sizes.at[giver].add(-shifted).at[sink].add(shifted)
    labels = jnp.searchsorted(jnp.cumsum(sizes), jnp.arange(rows * top), side="right").astype(jnp.int32)
    grid = labels.reshape(top, rows).T
    grid = grid[jax.random.permutation(jax.random.fold_in(own, 1), rows)]
    rotation = jax.random.randint(jax.random.fold_in(own, 2), (rows, 1), 0, top)
    return jnp.take_along_axis(grid, (jnp.arange(top)[None, :] + rotation) % top, axis=1)


def load_shares(number_of, total, reach, slope, full):
    loads = [(1 << 20) // math.isqrt(grade ** slope) + 1 for grade in range(1, number_of + 1)]
    largest = reach if full else min(reach, max(-(-total // number_of), total * loads[0] // sum(loads)))
    least = 1 if total - largest >= number_of - 1 else 0
    holding, rest = [largest] + [least] * (number_of - 1), total - largest - least * (number_of - 1)
    while rest > 0:
        free = [i for i in range(1, number_of) if holding[i] < largest] or [i for i in range(1, number_of) if holding[i] < reach]
        whole, left = sum([loads[i] for i in free]), rest
        for i in free:
            extra = min(reach - holding[i], max(1, left * loads[i] // whole), rest)
            holding[i] = holding[i] + extra
            rest = rest - extra
    return np.array(holding)


def bell_draw(own_key, shape, spread, most, cuts=(), kind=jnp.bfloat16):
    array = jax.random.normal(own_key, shape, jnp.float32) * spread
    if len(cuts) > 0:
        array = shard_levels(own_key, shape, cuts, -0.22, 0.18) * array
    return jnp.clip(array, min=-most, max=most).astype(kind)


def setup_inputs(seed: int = 0, part: int = 0) -> dict:
    seeds = jax.random.split(jax.random.key(seed), 13)
    part_splits = jax.random.split(jax.random.fold_in(seeds[12], part), 13)
    residual = bell_draw(part_splits[0], (TOKENS, D), 1.0, 6.0, ((0, 8), (1, 2)))
    norm_gain = jnp.clip(1.0 + 0.18 * jax.random.normal(seeds[1], (D,), jnp.float32), 0.099609375, 1.8984375).astype(jnp.bfloat16)
    router_weight = bell_draw(seeds[2], (D // SUB, EXPERTS), (D // SUB) ** -0.5, 0.25)
    expert_ids_keys = jax.random.split(jax.random.fold_in(part_splits[3], 1), TOKENS * SUB // (TOK_DEV * SUB))
    expert_ids_turns = jax.random.permutation(jax.random.fold_in(part_splits[3], 3), TOKENS * SUB // (TOK_DEV * SUB))
    expert_ids = jax.vmap(lambda own, number: assign_block(jax.random.fold_in(part_splits[3], 2), own, number, TOK_DEV * SUB, EXPERTS, TOP, CAP, 2))(expert_ids_keys, expert_ids_turns).reshape((TOKENS, SUB, TOP))
    expert_in = bell_draw(seeds[4], (EXPERTS, D // SUB, EFF), (D // SUB) ** -0.5, 0.25, ((0, 8), (2, 2)))
    expert_out = bell_draw(seeds[5], (EXPERTS, EFF, D // SUB), EFF ** -0.5, 0.15625, ((0, 8), (1, 2)))
    queries = draw_queries(jax.random.fold_in(jax.random.fold_in(seeds[12], part), 71), part)
    new_keys = draw_new_keys(jax.random.fold_in(jax.random.fold_in(seeds[12], part), 71), part)
    new_values = bell_draw(part_splits[8], (TOKENS, KV_HEADS * HD), 1.0, 6.0, ((0, 8), (1, 2)))
    cache_keys = draw_cache_keys(jax.random.fold_in(jax.random.fold_in(seeds[12], part), 71), part)
    cache_values = bell_draw(part_splits[10], (TOKENS, CACHE, KV_HEADS * HD), 1.0, 6.0, ((0, 8), (2, 2)))
    lengths = with_ends(jax.random.randint(part_splits[11], (TOKENS,), 1, CACHE + 1), jax.random.fold_in(part_splits[11], 1), 1, CACHE).astype(jnp.int32)
    return {"residual": residual, "norm_gain": norm_gain, "router_weight": router_weight, "expert_ids": expert_ids, "expert_in": expert_in, "expert_out": expert_out, "queries": queries, "new_keys": new_keys, "new_values": new_values, "cache_keys": cache_keys, "cache_values": cache_values, "lengths": lengths}


def normalize(residual, norm_gain):
    sub_width = D // SUB
    pieces = residual.astype(jnp.float32).reshape(residual.shape[0], -1, sub_width)
    gain_rows = norm_gain.astype(jnp.float32).reshape(-1, sub_width)
    meansq = lax.optimization_barrier(jnp.mean(pieces * pieces, axis=-1, keepdims=True))
    return (pieces * lax.rsqrt(meansq + 1e-06) * gain_rows).astype(jnp.bfloat16)

def route_weights(normed, router_weight, chosen_ids):
    logits = jnp.einsum('tsw,we->tse', normed.astype(jnp.float32), router_weight.astype(jnp.float32))
    onehot = (chosen_ids[..., None] == jnp.arange(EXPERTS, dtype=jnp.int32)).astype(jnp.float32)
    picked = lax.optimization_barrier(jnp.sum(onehot * logits[:, :, None, :], axis=-1))
    scores = jax.nn.sigmoid(picked)
    return scores / lax.optimization_barrier(jnp.sum(scores, axis=-1, keepdims=True))

def attend(queries, new_keys, new_values, cache_keys, cache_values, lengths):
    tokens = queries.shape[0]
    groups = KV_HEADS
    per_group = HEADS // KV_HEADS
    score_scale = 1.0 / math.sqrt(HD)
    query_heads = queries.astype(jnp.float32).reshape(tokens, groups, per_group, HD)
    keys_old = cache_keys.astype(jnp.float32).reshape(tokens, CACHE, groups, HD)
    values_old = cache_values.astype(jnp.float32).reshape(tokens, CACHE, groups, HD)
    keys_new = new_keys.astype(jnp.float32).reshape(tokens, groups, HD)
    values_new = new_values.astype(jnp.float32).reshape(tokens, groups, HD)
    scores = jnp.einsum('tgqd,tjgd->tgqj', query_heads, keys_old) * score_scale
    fresh_score = jnp.einsum('tgqd,tgd->tgq', query_heads, keys_new) * score_scale
    usable = (jnp.arange(CACHE, dtype=jnp.int32)[None, :] < lengths[:, None])[:, None, None, :]
    scores = jnp.where(usable, scores, -1e+30)
    row_max = jnp.maximum(lax.optimization_barrier(jnp.max(scores, axis=-1)), fresh_score)
    expo_old = jnp.where(usable, jnp.exp(scores - row_max[..., None]), 0.0)
    expo_new = jnp.exp(fresh_score - row_max)
    totals = lax.optimization_barrier(jnp.sum(expo_old, axis=-1)) + expo_new
    cache_probs = (expo_old / totals[..., None]).astype(jnp.bfloat16)
    fresh_probs = (expo_new / totals).astype(jnp.bfloat16)
    context = jnp.einsum('tgqj,tjgd->tgqd', cache_probs.astype(jnp.float32), values_old)
    context = context + fresh_probs.astype(jnp.float32)[..., None] * values_new[:, :, None, :]
    return context.reshape(tokens, D)

def reference(residual, norm_gain, router_weight, expert_ids, expert_in, expert_out, queries, new_keys, new_values, cache_keys, cache_values, lengths):
    sub_width = D // SUB
    normed = normalize(residual, norm_gain)
    weights = route_weights(normed, router_weight, expert_ids)
    flat_ids = expert_ids.reshape(-1).astype(jnp.int32)
    onehot = (flat_ids[:, None] == jnp.arange(EXPERTS, dtype=jnp.int32)[None, :]).astype(jnp.int32)
    before = jnp.cumsum(onehot, axis=0) - onehot
    slot_index = lax.optimization_barrier(jnp.sum(before * onehot, axis=1)).astype(jnp.int32)
    depth = N_EXPERT * CAP
    target = (flat_ids * depth + slot_index).astype(jnp.int32)
    sources = jnp.broadcast_to(normed[:, :, None, :], (TOKENS, SUB, TOP, sub_width)).reshape(-1, sub_width)
    buffer = jnp.zeros((EXPERTS * depth, sub_width), jnp.bfloat16).at[target].set(sources)
    buffer = buffer.reshape(EXPERTS, depth, sub_width)
    hidden = jax.nn.gelu(jnp.einsum('emw,ewf->emf', buffer.astype(jnp.float32), expert_in.astype(jnp.float32))).astype(jnp.bfloat16)
    output = jnp.einsum('emf,efw->emw', hidden.astype(jnp.float32), expert_out.astype(jnp.float32)).astype(jnp.bfloat16)
    picked = output.reshape(EXPERTS * depth, sub_width)[target].astype(jnp.float32)
    picked = picked.reshape(TOKENS, SUB, TOP, sub_width)
    moe = lax.optimization_barrier(jnp.sum(weights[..., None] * picked, axis=2)).reshape(TOKENS, D)
    context = attend(queries, new_keys, new_values, cache_keys, cache_values, lengths)
    attention = context.astype(jnp.bfloat16)
    mixed = (residual.astype(jnp.float32) + context + moe).astype(jnp.bfloat16)
    return (attention, mixed)
```

```python
import functools
import math

import jax
import jax.numpy as jnp
from jax import lax
from jax.experimental import pallas as pl
from jax.experimental.pallas import tpu as pltpu
from jax.sharding import PartitionSpec as P


D = 5120
SUB = 8
HEADS = 40
HD = 128
KV_HEADS = 8
EXPERTS = 128
TOP = 2
CAP = 5


BF16 = jnp.bfloat16
F32 = jnp.float32


def log2(value):
    bits = value.bit_length() - 1
    assert value == 1 << bits
    return bits


def in_vmem(kernel, out_shape, smem=(), plain=(), hbm=(), hbm_out=(), room=6 << 20, cost=1.0, **kwargs):
    def space(i, left):
        return pl.ANY if i in left else pltpu.SMEM if i in smem else pltpu.VMEM

    def call(*args):
        specs = [pl.BlockSpec(memory_space=space(i, hbm)) for i in range(len(args))]
        args = [
            pltpu.with_memory_space_constraint(
                a, pltpu.HBM if i in smem or i in plain or i in hbm else pltpu.VMEM
            )
            for i, a in enumerate(args)
        ]
        return pl.pallas_call(
            kernel,
            out_shape=tuple(
                jax.ShapeDtypeStruct(s.shape, s.dtype) if i in hbm_out else pltpu.VMEM(s.shape, s.dtype)
                for i, s in enumerate(out_shape)
            ),
            in_specs=specs,
            out_specs=tuple(
                pl.BlockSpec(memory_space=pl.ANY if i in hbm_out else pltpu.VMEM)
                for i in range(len(out_shape))
            ),
            compiler_params=pltpu.CompilerParams(vmem_limit_bytes=room),
            cost_estimate=pl.CostEstimate(
                flops=int(cost * 5e8), bytes_accessed=int(cost * 3e6), transcendentals=0
            ),
            **kwargs,
        )(*args)

    return call


def route_kernel(
    ids_ref, res_ref, gain_ref, pos_ref, sel_ref, normed_ref, *, sub_local, per_owner, n_owner
):
    owner = lax.axis_index("expert")
    mp = lax.axis_index("mp")
    tokens = ids_ref.shape[2]
    rows = tokens * SUB
    ids = jnp.concatenate([ids_ref[s].astype(F32) for s in range(SUB)], axis=0)
    ids = jnp.concatenate([ids, jnp.zeros((EXPERTS - SUB * TOP, tokens), F32)], axis=0)
    ids = jnp.concatenate([ids, jnp.zeros((EXPERTS, EXPERTS - tokens), F32)], axis=1).T
    expert_lane = lax.broadcasted_iota(jnp.int32, (tokens, EXPERTS), 1).astype(F32)

    def hot_rows(k):
        return jnp.concatenate(
            [
                (ids[0:tokens, s * TOP + k : s * TOP + k + 1] == expert_lane).astype(F32)
                for s in range(SUB)
            ],
            axis=0,
        )

    both = jnp.concatenate([hot_rows(k) for k in range(TOP)], axis=1)
    down = lax.broadcasted_iota(jnp.int32, (rows, rows), 0)
    across = lax.broadcasted_iota(jnp.int32, (rows, rows), 1)
    earlier = (across < down).astype(F32).astype(BF16)
    before = jnp.dot(earlier, both.astype(BF16), preferred_element_type=F32)
    lane = lax.broadcasted_iota(jnp.int32, (rows, EXPERTS), 1)
    lane_f = lane.astype(F32)
    total = jnp.zeros((1, EXPERTS), F32)
    packed = jnp.zeros((rows, EXPERTS), F32)
    half = n_owner // 2
    for k in range(TOP):
        hot = both[:, k * EXPERTS : (k + 1) * EXPERTS]
        ahead = before[:, k * EXPERTS : (k + 1) * EXPERTS] + total
        total = total + jnp.sum(hot, axis=0, keepdims=True)
        slot = jnp.sum(hot * ahead, axis=1, keepdims=True).astype(jnp.int32)
        expert = jnp.sum(hot * lane_f, axis=1, keepdims=True).astype(jnp.int32)
        apart = (expert >> log2(per_owner)) ^ owner
        block = ((apart & 1) ^ mp) * half + (apart >> 1)
        flat = (block * CAP + slot) * per_owner + (expert & (per_owner - 1))
        packed = jnp.where(lane == k, flat.astype(F32), packed)
        packed = jnp.where(lane == TOP + k, expert.astype(F32), packed)
    split = sub_local * tokens
    packed = jnp.where(
        mp == 0, packed, jnp.concatenate([packed[split:], packed[:split]], axis=0)
    )
    pos_ref[...] = packed
    turned = packed.T
    slots = sel_ref.shape[0]
    slot_row = lax.broadcasted_iota(jnp.int32, (slots, rows), 0).astype(F32)
    hit = slot_row == turned[0:1, :]
    for k in range(1, TOP):
        hit = hit | (slot_row == turned[k : k + 1, :])
    sel_ref[...] = hit.astype(F32).astype(BF16)
    width = res_ref.shape[1] // sub_local
    for s, piece in enumerate(normed_rows(res_ref, gain_ref, sub_local, width)):
        normed_ref[s * tokens : (s + 1) * tokens, :] = piece


def normed_rows(res_ref, gain_ref, sub_local, width):
    out = []
    chunks = width // HD
    for s in range(sub_local):
        piece = res_ref[:, s * width : (s + 1) * width].astype(F32)
        meansq = jnp.mean(piece * piece, axis=-1, keepdims=True)
        scaled = piece * lax.rsqrt(meansq + 1e-06)
        gained = [
            scaled[:, c * HD : (c + 1) * HD]
            * gain_ref[s * chunks + c : s * chunks + c + 1, :].astype(F32)
            for c in range(chunks)
        ]
        out.append(jnp.concatenate(gained, axis=1).astype(BF16))
    return out


def dispatch_kernel(normed_ref, peer_ref, peer_gain_ref, sel_ref, *out_refs, sub_local, width):
    rows = normed_rows(peer_ref, peer_gain_ref, sub_local, width)
    normed = jnp.concatenate([normed_ref[...]] + rows, axis=0)
    sent = jnp.dot(sel_ref[...], normed, preferred_element_type=F32).astype(BF16)
    slots = out_refs[0].shape[0]
    for j, ref in enumerate(out_refs):
        ref[...] = sent[j * slots : (j + 1) * slots]


def gate(normed, router, pos_ref, out_ref):
    logits = jnp.dot(normed, router, preferred_element_type=F32)
    rows = normed.shape[0]
    lane = lax.broadcasted_iota(jnp.int32, (rows, EXPERTS), 1)
    scores = []
    for k in range(TOP):
        expert = pos_ref[0:rows, TOP + k : TOP + k + 1].astype(jnp.int32)
        picked = jnp.sum(jnp.where(lane == expert, logits, 0.0), axis=1, keepdims=True)
        scores.append(jax.nn.sigmoid(picked))
    total = functools.reduce(lambda a, b: a + b, scores)
    out = jnp.zeros((rows, EXPERTS), F32)
    for k in range(TOP):
        out = jnp.where(lane == k, scores[k] / total, out)
    out_ref[...] = out


def combine_kernel(pos_ref, weight_ref, res_ref, context_ref, *refs, sub_local, width):
    blocks, out_ref = refs[:-1], refs[-1]
    tokens = res_ref.shape[0]
    rows = sub_local * tokens
    returned = jnp.concatenate([ref[...] for ref in blocks], axis=0)
    slots = returned.shape[0]
    lane = lax.broadcasted_iota(jnp.int32, (rows, slots), 1)
    moe = jnp.zeros((rows, width), F32)
    for k in range(TOP):
        flat = pos_ref[0:rows, k : k + 1].astype(jnp.int32)
        hot = (lane == flat).astype(F32).astype(BF16)
        picked = jnp.dot(hot, returned, preferred_element_type=F32)
        moe = moe + weight_ref[:, k : k + 1] * picked
    for s in range(sub_local):
        at = slice(s * width, (s + 1) * width)
        total = res_ref[:, at].astype(F32) + context_ref[:, at]
        out_ref[:, at] = (total + moe[s * tokens : (s + 1) * tokens]).astype(BF16)


def attend_kernel(
    length_ref,
    query_ref,
    key_ref,
    value_ref,
    cache_key_ref,
    cache_value_ref,
    normed_ref,
    router_ref,
    pos_ref,
    attention_ref,
    context_ref,
    gate_ref,
    spread_ref,
    gather_ref,
    new_key_ref,
    new_value_ref,
    rounded_ref,
    store_sem,
):
    tokens = query_ref.shape[0]
    unroll = math.gcd(tokens, 16)
    groups = key_ref.shape[1] // HD
    per_group = HEADS // KV_HEADS
    heads = groups * per_group
    pad = spread_ref.shape[0] // tokens
    cache_len = cache_key_ref.shape[1]
    scale = 1.0 / math.sqrt(HD)
    new_key_ref[...] = key_ref[...].astype(F32)
    new_value_ref[...] = value_ref[...].astype(F32)
    for h in range(heads, pad):
        spread_ref[pl.ds(h, tokens, stride=pad), :] = jnp.zeros((tokens, HD), F32)
    for h in range(heads):
        spread_ref[pl.ds(h, tokens, stride=pad), :] = query_ref[:, h * HD : (h + 1) * HD].astype(F32)
    lane = lax.broadcasted_iota(jnp.int32, (pad, cache_len), 1)
    row = lax.broadcasted_iota(jnp.int32, (pad, HD), 0)
    lane = lax.broadcasted_iota(jnp.int32, (pad, cache_len), 1)
    member = [(row >= g * per_group) & (row < (g + 1) * per_group) for g in range(groups)]

    def by_group(x):
        out = jnp.broadcast_to(x[:, 0:HD], (pad, HD))
        for g in range(1, groups):
            out = jnp.where(member[g], x[:, g * HD : (g + 1) * HD], out)
        return out

    for i in range(tokens // unroll):
        at = slice(i * unroll * pad, (i + 1) * unroll * pad)
        inner = [i * unroll + u for u in range(unroll)]
        queries = spread_ref[at, :]
        scores = []
        for u, t in enumerate(inner):
            own = queries[u * pad : (u + 1) * pad]
            query = jnp.concatenate([jnp.where(one, own, 0.0) for one in member], axis=1)
            scores.append(
                lax.dot_general(
                    query.astype(BF16),
                    cache_key_ref[t],
                    (((1,), (1,)), ((), ())),
                    preferred_element_type=F32,
                )
            )
        usable = jnp.concatenate([lane < length_ref[t] for t in inner], axis=0)
        scores = jnp.where(usable, jnp.concatenate(scores, axis=0) * scale, -1e30)
        new_key = jnp.concatenate([by_group(new_key_ref[t : t + 1, :]) for t in inner], axis=0)
        new_value = jnp.concatenate([by_group(new_value_ref[t : t + 1, :]) for t in inner], axis=0)
        fresh = jnp.sum(queries * new_key, axis=1, keepdims=True) * scale
        row_max = jnp.maximum(jnp.max(scores, axis=1, keepdims=True), fresh)
        expo = jnp.where(usable, jnp.exp(scores - row_max), 0.0)
        expo_new = jnp.exp(fresh - row_max)
        total = jnp.sum(expo, axis=1, keepdims=True) + expo_new
        probs = expo / total
        prob_new = (expo_new / total).astype(BF16).astype(F32)
        context = [
            by_group(
                jnp.dot(
                    probs[u * pad : (u + 1) * pad].astype(BF16),
                    cache_value_ref[t],
                    preferred_element_type=F32,
                )
            )
            for u, t in enumerate(inner)
        ]
        gather_ref[at, :] = jnp.concatenate(context, axis=0) + prob_new * new_value
    for h in range(heads):
        context = gather_ref[pl.ds(h, tokens, stride=pad), :]
        context_ref[:, h * HD : (h + 1) * HD] = context
        rounded_ref[:, h * HD : (h + 1) * HD] = context.astype(BF16)
    store = pltpu.make_async_copy(rounded_ref, attention_ref, store_sem)
    store.start()
    gate(normed_ref[...], router_ref[...], pos_ref, gate_ref)
    store.wait()


def ffn_kernel(*refs, n_block, per_owner):
    blocks = refs[:n_block]
    first_ref, second_ref, mine_ref, other_ref, rows_ref, out_ref = refs[n_block:]
    slots, width = blocks[0].shape
    lanes = range(width // HD)
    for b in range(n_block):
        block = blocks[b][...].astype(F32)
        for c in lanes:
            rows_ref[c, b * slots : (b + 1) * slots, :] = block[:, c * HD : (c + 1) * HD]
    depth = n_block * slots // per_owner
    at = [pl.ds(e, depth, stride=per_owner) for e in range(per_owner)]
    taken = [
        jnp.concatenate([rows_ref[c, a, :] for c in lanes], axis=1).astype(BF16) for a in at
    ]
    hidden = [
        jnp.dot(x, first_ref[e], preferred_element_type=F32) for e, x in enumerate(taken)
    ]
    hidden = [jax.nn.gelu(h).astype(BF16) for h in hidden]
    for e, h in enumerate(hidden):
        result = jnp.dot(h, second_ref[e], preferred_element_type=F32)
        for c in lanes:
            out_ref[c, at[e], :] = result[:, c * HD : (c + 1) * HD]
    split = n_block // 2 * slots
    for c in lanes:
        mine_ref[:, c * HD : (c + 1) * HD] = out_ref[c, 0:split, :]
        other_ref[:, c * HD : (c + 1) * HD] = out_ref[c, split : 2 * split, :].astype(BF16)


def reduce_kernel(mine_ref, other_ref, *out_refs):
    slots = out_refs[0].shape[0]
    for j, ref in enumerate(out_refs):
        at = slice(j * slots, (j + 1) * slots)
        ref[...] = (mine_ref[at, :] + other_ref[at, :].astype(F32)).astype(BF16)


def per_device(
    residual,
    norm_gain,
    router_weight,
    expert_ids,
    expert_in,
    expert_out,
    queries,
    new_keys,
    new_values,
    cache_keys,
    cache_values,
    lengths,
):
    width = D // SUB
    tokens = residual.shape[0]
    sub_local = residual.shape[1] // width
    n_owner = lax.axis_size("expert")
    n_mp = lax.axis_size("mp")
    assert n_mp == 2
    per_owner = expert_in.shape[0]
    slots = CAP * per_owner
    half = n_owner // 2
    rows = tokens * SUB
    gain = norm_gain.reshape(-1, HD)

    swap = [(0, 1), (1, 0)]
    order = sorted(range(half), key=lambda j: (-j.bit_length(), j))

    def partners(j):
        return [
            (e * n_mp + m, (e ^ (2 * j + m)) * n_mp + m) for e in range(n_owner) for m in range(n_mp)
        ]

    peer_residual = lax.ppermute(residual, "mp", swap)
    peer_gain = lax.ppermute(gain, "mp", swap)
    pos, sel, normed = in_vmem(
        functools.partial(route_kernel, sub_local=sub_local, per_owner=per_owner, n_owner=n_owner),
        (
            jax.ShapeDtypeStruct((rows, EXPERTS), F32),
            jax.ShapeDtypeStruct((half * slots, rows), BF16),
            jax.ShapeDtypeStruct((sub_local * tokens, width), BF16),
        ),
        plain=(0, 1, 2),
        cost=20.0,
        name="route",
    )(expert_ids.transpose(1, 2, 0), residual, gain)
    sent = in_vmem(
        functools.partial(dispatch_kernel, sub_local=sub_local, width=width),
        tuple(jax.ShapeDtypeStruct((slots, width), BF16) for _ in range(half)),
        cost=20.0,
        name="dispatch",
    )(normed, peer_residual, peer_gain, sel)

    own = [None] * half
    for j in order:
        own[j] = lax.ppermute(sent[j], ("expert", "mp"), partners(j))
    groups = new_keys.shape[1] // HD
    pad = -(-groups * (HEADS // KV_HEADS) // 8) * 8
    attention, context, weights = in_vmem(
        attend_kernel,
        (
            jax.ShapeDtypeStruct(queries.shape, BF16),
            jax.ShapeDtypeStruct(queries.shape, F32),
            jax.ShapeDtypeStruct((sub_local * tokens, EXPERTS), F32),
        ),
        smem=(0,),
        hbm_out=(0,),
        scratch_shapes=(
            pltpu.VMEM((tokens * pad, HD), F32),
            pltpu.VMEM((tokens * pad, HD), F32),
            pltpu.VMEM(new_keys.shape, F32),
            pltpu.VMEM(new_values.shape, F32),
            pltpu.VMEM(queries.shape, BF16),
            pltpu.SemaphoreType.DMA,
        ),
        cost=4.0,
        name="attend",
    )(
        lengths,
        queries,
        new_keys,
        new_values,
        cache_keys,
        cache_values,
        normed,
        router_weight,
        pos,
    )
    peer = [lax.ppermute(block, "mp", swap) for block in own]

    mine, other = in_vmem(
        functools.partial(ffn_kernel, n_block=n_owner, per_owner=per_owner),
        (
            jax.ShapeDtypeStruct((half * slots, width), F32),
            jax.ShapeDtypeStruct((half * slots, width), BF16),
        ),
        scratch_shapes=(
            pltpu.VMEM((width // HD, n_owner * slots, HD), F32),
            pltpu.VMEM((width // HD, n_owner * slots, HD), F32),
        ),
        room=12 << 20,
        cost=5.0,
        name="ffn",
    )(*own, *peer, expert_in, expert_out)
    result = in_vmem(
        reduce_kernel,
        tuple(jax.ShapeDtypeStruct((slots, width), BF16) for _ in range(half)),
        name="reduce",
    )(mine, lax.ppermute(other, "mp", swap))

    back = [None] * half
    for j in order:
        back[j] = lax.ppermute(result[j], ("expert", "mp"), partners(j))
    peer_back = [lax.ppermute(block, "mp", swap) for block in back]
    (mixed,) = in_vmem(
        functools.partial(combine_kernel, sub_local=sub_local, width=width),
        (jax.ShapeDtypeStruct(residual.shape, BF16),),
        name="combine",
    )(pos, weights, residual, context, *back, *peer_back)
    return (attention, mixed)


def solution(mesh):
    placed = (
        P(("groups", "expert"), "mp"),
        P("mp"),
        P(),
        P(("groups", "expert"), None, None),
        P("expert", None, "mp"),
        P("expert", "mp", None),
        P(("groups", "expert"), "mp"),
        P(("groups", "expert"), "mp"),
        P(("groups", "expert"), "mp"),
        P(("groups", "expert"), None, "mp"),
        P(("groups", "expert"), None, "mp"),
        P(("groups", "expert")),
    )
    return jax.shard_map(
        per_device,
        mesh=mesh,
        in_specs=placed,
        out_specs=(P(("groups", "expert"), "mp"), P(("groups", "expert"), "mp")),
        check_vma=False,
    )
```

```python
import functools
import math

import jax
import jax.numpy as jnp
from jax import lax
from jax.experimental import pallas as pl
from jax.experimental.pallas import tpu as pltpu
from jax.sharding import PartitionSpec as P


D = 5120
SUB = 8
HEADS = 40
HD = 128
KV_HEADS = 8
EXPERTS = 128
TOP = 2
CAP = 5


BF16 = jnp.bfloat16
F32 = jnp.float32


def log2(value):
    bits = value.bit_length() - 1
    assert value == 1 << bits
    return bits


def in_vmem(kernel, out_shape, smem=(), plain=(), hbm=(), hbm_out=(), room=6 << 20, cost=1.0, **kwargs):
    def space(i, left):
        return pl.ANY if i in left else pltpu.SMEM if i in smem else pltpu.VMEM

    def call(*args):
        specs = [pl.BlockSpec(memory_space=space(i, hbm)) for i in range(len(args))]
        args = [
            pltpu.with_memory_space_constraint(
                a, pltpu.HBM if i in smem or i in plain or i in hbm else pltpu.VMEM
            )
            for i, a in enumerate(args)
        ]
        return pl.pallas_call(
            kernel,
            out_shape=tuple(
                jax.ShapeDtypeStruct(s.shape, s.dtype) if i in hbm_out else pltpu.VMEM(s.shape, s.dtype)
                for i, s in enumerate(out_shape)
            ),
            in_specs=specs,
            out_specs=tuple(
                pl.BlockSpec(memory_space=pl.ANY if i in hbm_out else pltpu.VMEM)
                for i in range(len(out_shape))
            ),
            compiler_params=pltpu.CompilerParams(vmem_limit_bytes=room),
            cost_estimate=pl.CostEstimate(
                flops=int(cost * 5e8), bytes_accessed=int(cost * 3e6), transcendentals=0
            ),
            **kwargs,
        )(*args)

    return call


def ring_place(pair, count):
    return jnp.where((pair & 1) == 0, pair >> 1, count - 1 - (pair >> 1))


def route_kernel(
    ids_hbm_ref,
    res_hbm_ref,
    gain_hbm_ref,
    pos_ref,
    sel_ref,
    normed_ref,
    ids_ref,
    res_ref,
    gain_ref,
    sem,
    *,
    sub_local,
    per_owner,
    n_owner,
):
    fetches = [
        pltpu.make_async_copy(source, target, sem.at[i])
        for i, (source, target) in enumerate(
            [(ids_hbm_ref, ids_ref), (res_hbm_ref, res_ref), (gain_hbm_ref, gain_ref)]
        )
    ]
    for fetch in fetches:
        fetch.start()
    owner = lax.axis_index("expert")
    mp = lax.axis_index("mp")
    tokens = ids_ref.shape[2]
    rows = tokens * SUB
    fetches[0].wait()
    ids = jnp.concatenate([ids_ref[s].astype(F32) for s in range(SUB)], axis=0)
    ids = jnp.concatenate([ids, jnp.zeros((EXPERTS - SUB * TOP, tokens), F32)], axis=0)
    ids = jnp.concatenate([ids, jnp.zeros((EXPERTS, EXPERTS - tokens), F32)], axis=1).T
    expert_lane = lax.broadcasted_iota(jnp.int32, (tokens, EXPERTS), 1).astype(F32)

    def hot_rows(k):
        return jnp.concatenate(
            [
                (ids[0:tokens, s * TOP + k : s * TOP + k + 1] == expert_lane).astype(F32)
                for s in range(SUB)
            ],
            axis=0,
        )

    both = jnp.concatenate([hot_rows(k) for k in range(TOP)], axis=1)
    down = lax.broadcasted_iota(jnp.int32, (rows, rows), 0)
    across = lax.broadcasted_iota(jnp.int32, (rows, rows), 1)
    earlier = (across < down).astype(F32).astype(BF16)
    before = jnp.dot(earlier, both.astype(BF16), preferred_element_type=F32)
    lane = lax.broadcasted_iota(jnp.int32, (rows, EXPERTS), 1)
    lane_f = lane.astype(F32)
    total = jnp.zeros((1, EXPERTS), F32)
    packed = jnp.zeros((rows, EXPERTS), F32)
    half = n_owner // 2
    for k in range(TOP):
        hot = both[:, k * EXPERTS : (k + 1) * EXPERTS]
        ahead = before[:, k * EXPERTS : (k + 1) * EXPERTS] + total
        total = total + jnp.sum(hot, axis=0, keepdims=True)
        slot = jnp.sum(hot * ahead, axis=1, keepdims=True).astype(jnp.int32)
        expert = jnp.sum(hot * lane_f, axis=1, keepdims=True).astype(jnp.int32)
        target = expert >> log2(per_owner)
        step = (ring_place(target >> 1, half) - ring_place(owner >> 1, half)) & (half - 1)
        block = ((target ^ owner ^ mp) & 1) * half + step
        flat = (block * CAP + slot) * per_owner + (expert & (per_owner - 1))
        packed = jnp.where(lane == k, flat.astype(F32), packed)
        packed = jnp.where(lane == TOP + k, expert.astype(F32), packed)
    split = sub_local * tokens
    packed = jnp.where(
        mp == 0, packed, jnp.concatenate([packed[split:], packed[:split]], axis=0)
    )
    pos_ref[...] = packed
    turned = packed.T
    slots = sel_ref.shape[0]
    slot_row = lax.broadcasted_iota(jnp.int32, (slots, rows), 0).astype(F32)
    hit = slot_row == turned[0:1, :]
    for k in range(1, TOP):
        hit = hit | (slot_row == turned[k : k + 1, :])
    sel_ref[...] = hit.astype(F32).astype(BF16)
    width = res_ref.shape[1] // sub_local
    fetches[1].wait()
    fetches[2].wait()
    for s, piece in enumerate(normed_rows(res_ref, gain_ref, sub_local, width)):
        normed_ref[s * tokens : (s + 1) * tokens, :] = piece


def normed_rows(res_ref, gain_ref, sub_local, width):
    out = []
    chunks = width // HD
    for s in range(sub_local):
        piece = res_ref[:, s * width : (s + 1) * width].astype(F32)
        meansq = jnp.mean(piece * piece, axis=-1, keepdims=True)
        scaled = piece * lax.rsqrt(meansq + 1e-06)
        gained = [
            scaled[:, c * HD : (c + 1) * HD]
            * gain_ref[s * chunks + c : s * chunks + c + 1, :].astype(F32)
            for c in range(chunks)
        ]
        out.append(jnp.concatenate(gained, axis=1).astype(BF16))
    return out


def dispatch_kernel(normed_ref, peer_ref, peer_gain_ref, sel_ref, *out_refs, sub_local, width):
    rows = normed_rows(peer_ref, peer_gain_ref, sub_local, width)
    normed = jnp.concatenate([normed_ref[...]] + rows, axis=0)
    sent = jnp.dot(sel_ref[...], normed, preferred_element_type=F32).astype(BF16)
    slots = out_refs[0].shape[0]
    for j, ref in enumerate(out_refs):
        ref[...] = sent[j * slots : (j + 1) * slots]


def gate(normed, router, pos_ref, out_ref):
    logits = jnp.dot(normed, router, preferred_element_type=F32)
    rows = normed.shape[0]
    lane = lax.broadcasted_iota(jnp.int32, (rows, EXPERTS), 1)
    scores = []
    for k in range(TOP):
        expert = pos_ref[0:rows, TOP + k : TOP + k + 1].astype(jnp.int32)
        picked = jnp.sum(jnp.where(lane == expert, logits, 0.0), axis=1, keepdims=True)
        scores.append(jax.nn.sigmoid(picked))
    total = functools.reduce(lambda a, b: a + b, scores)
    out = jnp.zeros((rows, EXPERTS), F32)
    for k in range(TOP):
        out = jnp.where(lane == k, scores[k] / total, out)
    out_ref[...] = out


def combine_kernel(pos_ref, weight_ref, res_ref, context_ref, *refs, sub_local, width):
    blocks, (out_hbm_ref, out_ref, sem) = refs[:-3], refs[-3:]
    tokens = res_ref.shape[0]
    rows = sub_local * tokens
    returned = jnp.concatenate([ref[...] for ref in blocks], axis=0)
    slots = returned.shape[0]
    lane = lax.broadcasted_iota(jnp.int32, (rows, slots), 1)
    moe = jnp.zeros((rows, width), F32)
    for k in range(TOP):
        flat = pos_ref[0:rows, k : k + 1].astype(jnp.int32)
        hot = (lane == flat).astype(F32).astype(BF16)
        picked = jnp.dot(hot, returned, preferred_element_type=F32)
        moe = moe + weight_ref[:, k : k + 1] * picked
    stores = []
    for s in range(sub_local):
        at = slice(s * width, (s + 1) * width)
        total = res_ref[:, at].astype(F32) + context_ref[:, at]
        out_ref[:, at] = (total + moe[s * tokens : (s + 1) * tokens]).astype(BF16)
        stores.append(pltpu.make_async_copy(out_ref.at[:, at], out_hbm_ref.at[:, at], sem.at[s]))
        stores[-1].start()
    for store in stores:
        store.wait()


def attend_kernel(
    length_ref,
    query_ref,
    key_ref,
    value_ref,
    cache_key_ref,
    cache_value_ref,
    normed_ref,
    router_ref,
    pos_ref,
    attention_ref,
    context_ref,
    gate_ref,
    spread_ref,
    gather_ref,
    new_key_ref,
    new_value_ref,
    rounded_ref,
    store_sem,
):
    tokens = query_ref.shape[0]
    unroll = math.gcd(tokens, 16)
    groups = key_ref.shape[1] // HD
    per_group = HEADS // KV_HEADS
    heads = groups * per_group
    pad = spread_ref.shape[0] // tokens
    cache_len = cache_key_ref.shape[1]
    scale = 1.0 / math.sqrt(HD)
    new_key_ref[...] = key_ref[...].astype(F32)
    new_value_ref[...] = value_ref[...].astype(F32)
    for h in range(heads, pad):
        spread_ref[pl.ds(h, tokens, stride=pad), :] = jnp.zeros((tokens, HD), F32)
    for h in range(heads):
        spread_ref[pl.ds(h, tokens, stride=pad), :] = query_ref[:, h * HD : (h + 1) * HD].astype(F32)
    lane = lax.broadcasted_iota(jnp.int32, (pad, cache_len), 1)
    row = lax.broadcasted_iota(jnp.int32, (pad, HD), 0)
    lane = lax.broadcasted_iota(jnp.int32, (pad, cache_len), 1)
    member = [(row >= g * per_group) & (row < (g + 1) * per_group) for g in range(groups)]

    def by_group(x):
        out = jnp.broadcast_to(x[:, 0:HD], (pad, HD))
        for g in range(1, groups):
            out = jnp.where(member[g], x[:, g * HD : (g + 1) * HD], out)
        return out

    for i in range(tokens // unroll):
        at = slice(i * unroll * pad, (i + 1) * unroll * pad)
        inner = [i * unroll + u for u in range(unroll)]
        queries = spread_ref[at, :]
        scores = []
        for u, t in enumerate(inner):
            own = queries[u * pad : (u + 1) * pad]
            query = jnp.concatenate([jnp.where(one, own, 0.0) for one in member], axis=1)
            scores.append(
                lax.dot_general(
                    query.astype(BF16),
                    cache_key_ref[t],
                    (((1,), (1,)), ((), ())),
                    preferred_element_type=F32,
                )
            )
        usable = jnp.concatenate([lane < length_ref[t] for t in inner], axis=0)
        scores = jnp.where(usable, jnp.concatenate(scores, axis=0) * scale, -1e30)
        new_key = jnp.concatenate([by_group(new_key_ref[t : t + 1, :]) for t in inner], axis=0)
        new_value = jnp.concatenate([by_group(new_value_ref[t : t + 1, :]) for t in inner], axis=0)
        fresh = jnp.sum(queries * new_key, axis=1, keepdims=True) * scale
        row_max = jnp.maximum(jnp.max(scores, axis=1, keepdims=True), fresh)
        expo = jnp.where(usable, jnp.exp(scores - row_max), 0.0)
        expo_new = jnp.exp(fresh - row_max)
        total = jnp.sum(expo, axis=1, keepdims=True) + expo_new
        probs = expo / total
        prob_new = (expo_new / total).astype(BF16).astype(F32)
        context = [
            by_group(
                jnp.dot(
                    probs[u * pad : (u + 1) * pad].astype(BF16),
                    cache_value_ref[t],
                    preferred_element_type=F32,
                )
            )
            for u, t in enumerate(inner)
        ]
        gather_ref[at, :] = jnp.concatenate(context, axis=0) + prob_new * new_value
    for h in range(heads):
        context = gather_ref[pl.ds(h, tokens, stride=pad), :]
        context_ref[:, h * HD : (h + 1) * HD] = context
        rounded_ref[:, h * HD : (h + 1) * HD] = context.astype(BF16)
    store = pltpu.make_async_copy(rounded_ref, attention_ref, store_sem)
    store.start()
    gate(normed_ref[...], router_ref[...], pos_ref, gate_ref)
    store.wait()


def ffn_kernel(*refs, n_block, per_owner):
    blocks = refs[:n_block]
    first_ref, second_ref, mine_ref, other_ref, rows_ref, out_ref = refs[n_block:]
    slots, width = blocks[0].shape
    lanes = range(width // HD)
    for b in range(n_block):
        block = blocks[b][...].astype(F32)
        for c in lanes:
            rows_ref[c, b * slots : (b + 1) * slots, :] = block[:, c * HD : (c + 1) * HD]
    depth = n_block * slots // per_owner
    at = [pl.ds(e, depth, stride=per_owner) for e in range(per_owner)]
    taken = [
        jnp.concatenate([rows_ref[c, a, :] for c in lanes], axis=1).astype(BF16) for a in at
    ]
    hidden = [
        jnp.dot(x, first_ref[e], preferred_element_type=F32) for e, x in enumerate(taken)
    ]
    hidden = [jax.nn.gelu(h).astype(BF16) for h in hidden]
    for e, h in enumerate(hidden):
        result = jnp.dot(h, second_ref[e], preferred_element_type=F32)
        for c in lanes:
            out_ref[c, at[e], :] = result[:, c * HD : (c + 1) * HD]
    split = n_block // 2 * slots
    for c in lanes:
        mine_ref[:, c * HD : (c + 1) * HD] = out_ref[c, 0:split, :]
        other_ref[:, c * HD : (c + 1) * HD] = out_ref[c, split : 2 * split, :].astype(BF16)


def reduce_kernel(mine_ref, other_ref, *out_refs):
    slots = out_refs[0].shape[0]
    for j, ref in enumerate(out_refs):
        at = slice(j * slots, (j + 1) * slots)
        ref[...] = (mine_ref[at, :] + other_ref[at, :].astype(F32)).astype(BF16)


def per_device(
    residual,
    norm_gain,
    router_weight,
    expert_ids,
    expert_in,
    expert_out,
    queries,
    new_keys,
    new_values,
    cache_keys,
    cache_values,
    lengths,
):
    width = D // SUB
    tokens = residual.shape[0]
    sub_local = residual.shape[1] // width
    n_owner = lax.axis_size("expert")
    n_mp = lax.axis_size("mp")
    assert n_mp == 2
    per_owner = expert_in.shape[0]
    slots = CAP * per_owner
    half = n_owner // 2
    rows = tokens * SUB
    gain = norm_gain.reshape(-1, HD)

    swap = [(0, 1), (1, 0)]
    order = [half // 2] + [j for j in range(1, half) if j != half // 2] + [0]
    ring = list(range(0, half, 2)) + list(range(1, half, 2))[::-1]

    def partners(j, back=False):
        pairs = []
        for e in range(n_owner):
            far = ring[(ring.index(e >> 1) + j) % half]
            for m in range(n_mp):
                pair = (e * n_mp + m, (2 * far + ((e ^ m) & 1)) * n_mp + m)
                pairs.append(pair[::-1] if back else pair)
        return pairs

    peer_residual = lax.ppermute(residual, "mp", swap)
    peer_gain = lax.ppermute(gain, "mp", swap)
    pos, sel, normed = in_vmem(
        functools.partial(route_kernel, sub_local=sub_local, per_owner=per_owner, n_owner=n_owner),
        (
            jax.ShapeDtypeStruct((rows, EXPERTS), F32),
            jax.ShapeDtypeStruct((half * slots, rows), BF16),
            jax.ShapeDtypeStruct((sub_local * tokens, width), BF16),
        ),
        hbm=(0, 1, 2),
        scratch_shapes=(
            pltpu.VMEM((SUB, TOP, tokens), jnp.int32),
            pltpu.VMEM(residual.shape, BF16),
            pltpu.VMEM(gain.shape, BF16),
            pltpu.SemaphoreType.DMA((3,)),
        ),
        cost=20.0,
        name="route",
    )(expert_ids.transpose(1, 2, 0), residual, gain)
    sent = in_vmem(
        functools.partial(dispatch_kernel, sub_local=sub_local, width=width),
        tuple(jax.ShapeDtypeStruct((slots, width), BF16) for _ in range(half)),
        cost=20.0,
        name="dispatch",
    )(normed, peer_residual, peer_gain, sel)

    own = [None] * half
    for j in order:
        own[j] = lax.ppermute(sent[j], ("expert", "mp"), partners(j))
    groups = new_keys.shape[1] // HD
    pad = -(-groups * (HEADS // KV_HEADS) // 8) * 8
    attention, context, weights = in_vmem(
        attend_kernel,
        (
            jax.ShapeDtypeStruct(queries.shape, BF16),
            jax.ShapeDtypeStruct(queries.shape, F32),
            jax.ShapeDtypeStruct((sub_local * tokens, EXPERTS), F32),
        ),
        smem=(0,),
        hbm_out=(0,),
        scratch_shapes=(
            pltpu.VMEM((tokens * pad, HD), F32),
            pltpu.VMEM((tokens * pad, HD), F32),
            pltpu.VMEM(new_keys.shape, F32),
            pltpu.VMEM(new_values.shape, F32),
            pltpu.VMEM(queries.shape, BF16),
            pltpu.SemaphoreType.DMA,
        ),
        cost=4.0,
        name="attend",
    )(
        lengths,
        queries,
        new_keys,
        new_values,
        cache_keys,
        cache_values,
        normed,
        router_weight,
        pos,
    )
    peer = [None] * half
    for j in order:
        peer[j] = lax.ppermute(own[j], "mp", swap)

    def expert_pass(chosen, name):
        mine, other = in_vmem(
            functools.partial(ffn_kernel, n_block=2 * len(chosen), per_owner=per_owner),
            (
                jax.ShapeDtypeStruct((len(chosen) * slots, width), F32),
                jax.ShapeDtypeStruct((len(chosen) * slots, width), BF16),
            ),
            scratch_shapes=(
                pltpu.VMEM((width // HD, 2 * len(chosen) * slots, HD), F32),
                pltpu.VMEM((width // HD, 2 * len(chosen) * slots, HD), F32),
            ),
            room=12 << 20,
            cost=5.0,
            name=name,
        )(*[own[j] for j in chosen], *[peer[j] for j in chosen], expert_in, expert_out)
        return in_vmem(
            reduce_kernel,
            tuple(jax.ShapeDtypeStruct((slots, width), BF16) for _ in chosen),
            name="reduce",
        )(mine, lax.ppermute(other, "mp", swap))

    back = [None] * half
    early = order[: half // 2]
    late = order[half // 2 :]
    for chosen, name in ((early, "ffn_first"), (late, "ffn_last")):
        for j, block in zip(chosen, expert_pass(chosen, name)):
            back[j] = lax.ppermute(block, ("expert", "mp"), partners(j, back=True))
    peer_back = [None] * half
    for j in order:
        peer_back[j] = lax.ppermute(back[j], "mp", swap)
    (mixed,) = in_vmem(
        functools.partial(combine_kernel, sub_local=sub_local, width=width),
        (jax.ShapeDtypeStruct(residual.shape, BF16),),
        hbm_out=(0,),
        scratch_shapes=(
            pltpu.VMEM(residual.shape, BF16),
            pltpu.SemaphoreType.DMA((sub_local,)),
        ),
        name="combine",
    )(pos, weights, residual, context, *back, *peer_back)
    return (attention, mixed)


def solution(mesh):
    placed = (
        P(("groups", "expert"), "mp"),
        P("mp"),
        P(),
        P(("groups", "expert"), None, None),
        P("expert", None, "mp"),
        P("expert", "mp", None),
        P(("groups", "expert"), "mp"),
        P(("groups", "expert"), "mp"),
        P(("groups", "expert"), "mp"),
        P(("groups", "expert"), None, "mp"),
        P(("groups", "expert"), None, "mp"),
        P(("groups", "expert")),
    )
    return jax.shard_map(
        per_device,
        mesh=mesh,
        in_specs=placed,
        out_specs=(P(("groups", "expert"), "mp"), P(("groups", "expert"), "mp")),
        check_vma=False,
    )
```

```python
import functools
import math

import jax
import jax.numpy as jnp
from jax import lax
from jax.experimental import pallas as pl
from jax.experimental.pallas import tpu as pltpu
from jax.sharding import PartitionSpec as P


D = 5120
SUB = 8
HEADS = 40
HD = 128
KV_HEADS = 8
EXPERTS = 128
TOP = 2
CAP = 5


BF16 = jnp.bfloat16
F32 = jnp.float32


def log2(value):
    bits = value.bit_length() - 1
    assert value == 1 << bits
    return bits


def in_vmem(kernel, out_shape, smem=(), plain=(), hbm=(), hbm_out=(), room=6 << 20, cost=1.0, **kwargs):
    def space(i, left):
        return pl.ANY if i in left else pltpu.SMEM if i in smem else pltpu.VMEM

    def call(*args):
        specs = [pl.BlockSpec(memory_space=space(i, hbm)) for i in range(len(args))]
        args = [
            pltpu.with_memory_space_constraint(
                a, pltpu.HBM if i in smem or i in plain or i in hbm else pltpu.VMEM
            )
            for i, a in enumerate(args)
        ]
        return pl.pallas_call(
            kernel,
            out_shape=tuple(
                jax.ShapeDtypeStruct(s.shape, s.dtype) if i in hbm_out else pltpu.VMEM(s.shape, s.dtype)
                for i, s in enumerate(out_shape)
            ),
            in_specs=specs,
            out_specs=tuple(
                pl.BlockSpec(memory_space=pl.ANY if i in hbm_out else pltpu.VMEM)
                for i in range(len(out_shape))
            ),
            compiler_params=pltpu.CompilerParams(vmem_limit_bytes=room),
            cost_estimate=pl.CostEstimate(
                flops=int(cost * 5e8), bytes_accessed=int(cost * 3e6), transcendentals=0
            ),
            **kwargs,
        )(*args)

    return call


def ring_place(pair, count):
    return jnp.where((pair & 1) == 0, pair >> 1, count - 1 - (pair >> 1))


def route_kernel(
    ids_hbm_ref,
    res_hbm_ref,
    gain_hbm_ref,
    pos_ref,
    sel_ref,
    normed_ref,
    ids_ref,
    res_ref,
    gain_ref,
    sem,
    *,
    sub_local,
    per_owner,
    n_owner,
):
    fetches = [
        pltpu.make_async_copy(source, target, sem.at[i])
        for i, (source, target) in enumerate(
            [(ids_hbm_ref, ids_ref), (res_hbm_ref, res_ref), (gain_hbm_ref, gain_ref)]
        )
    ]
    for fetch in fetches:
        fetch.start()
    owner = lax.axis_index("expert")
    mp = lax.axis_index("mp")
    tokens = ids_ref.shape[2]
    rows = tokens * SUB
    fetches[0].wait()
    ids = jnp.concatenate([ids_ref[s].astype(F32) for s in range(SUB)], axis=0)
    ids = jnp.concatenate([ids, jnp.zeros((EXPERTS - SUB * TOP, tokens), F32)], axis=0)
    ids = jnp.concatenate([ids, jnp.zeros((EXPERTS, EXPERTS - tokens), F32)], axis=1).T
    expert_lane = lax.broadcasted_iota(jnp.int32, (tokens, EXPERTS), 1).astype(F32)

    def hot_rows(k):
        return jnp.concatenate(
            [
                (ids[0:tokens, s * TOP + k : s * TOP + k + 1] == expert_lane).astype(F32)
                for s in range(SUB)
            ],
            axis=0,
        )

    both = jnp.concatenate([hot_rows(k) for k in range(TOP)], axis=1)
    down = lax.broadcasted_iota(jnp.int32, (rows, rows), 0)
    across = lax.broadcasted_iota(jnp.int32, (rows, rows), 1)
    earlier = (across < down).astype(F32).astype(BF16)
    before = jnp.dot(earlier, both.astype(BF16), preferred_element_type=F32)
    lane = lax.broadcasted_iota(jnp.int32, (rows, EXPERTS), 1)
    lane_f = lane.astype(F32)
    total = jnp.zeros((1, EXPERTS), F32)
    packed = jnp.zeros((rows, EXPERTS), F32)
    half = n_owner // 2
    for k in range(TOP):
        hot = both[:, k * EXPERTS : (k + 1) * EXPERTS]
        ahead = before[:, k * EXPERTS : (k + 1) * EXPERTS] + total
        total = total + jnp.sum(hot, axis=0, keepdims=True)
        slot = jnp.sum(hot * ahead, axis=1, keepdims=True).astype(jnp.int32)
        expert = jnp.sum(hot * lane_f, axis=1, keepdims=True).astype(jnp.int32)
        target = expert >> log2(per_owner)
        step = (ring_place(target >> 1, half) - ring_place(owner >> 1, half)) & (half - 1)
        block = ((target ^ owner ^ mp) & 1) * half + step
        flat = (block * CAP + slot) * per_owner + (expert & (per_owner - 1))
        packed = jnp.where(lane == k, flat.astype(F32), packed)
        packed = jnp.where(lane == TOP + k, expert.astype(F32), packed)
    split = sub_local * tokens
    packed = jnp.where(
        mp == 0, packed, jnp.concatenate([packed[split:], packed[:split]], axis=0)
    )
    pos_ref[...] = packed
    turned = packed.T
    slots = sel_ref.shape[0]
    slot_row = lax.broadcasted_iota(jnp.int32, (slots, rows), 0).astype(F32)
    hit = slot_row == turned[0:1, :]
    for k in range(1, TOP):
        hit = hit | (slot_row == turned[k : k + 1, :])
    sel_ref[...] = hit.astype(F32).astype(BF16)
    width = res_ref.shape[1] // sub_local
    fetches[1].wait()
    fetches[2].wait()
    for s, piece in enumerate(normed_rows(res_ref, gain_ref, sub_local, width)):
        normed_ref[s * tokens : (s + 1) * tokens, :] = piece


def normed_rows(res_ref, gain_ref, sub_local, width):
    out = []
    chunks = width // HD
    for s in range(sub_local):
        piece = res_ref[:, s * width : (s + 1) * width].astype(F32)
        meansq = jnp.mean(piece * piece, axis=-1, keepdims=True)
        scaled = piece * lax.rsqrt(meansq + 1e-06)
        gained = [
            scaled[:, c * HD : (c + 1) * HD]
            * gain_ref[s * chunks + c : s * chunks + c + 1, :].astype(F32)
            for c in range(chunks)
        ]
        out.append(jnp.concatenate(gained, axis=1).astype(BF16))
    return out


def dispatch_kernel(normed_ref, peer_ref, peer_gain_ref, sel_ref, *out_refs, sub_local, width):
    rows = normed_rows(peer_ref, peer_gain_ref, sub_local, width)
    normed = jnp.concatenate([normed_ref[...]] + rows, axis=0)
    sent = jnp.dot(sel_ref[...], normed, preferred_element_type=F32).astype(BF16)
    slots = out_refs[0].shape[0]
    for j, ref in enumerate(out_refs):
        ref[...] = sent[j * slots : (j + 1) * slots]


def gate(normed, router, pos_ref, out_ref):
    logits = jnp.dot(normed, router, preferred_element_type=F32)
    rows = normed.shape[0]
    lane = lax.broadcasted_iota(jnp.int32, (rows, EXPERTS), 1)
    scores = []
    for k in range(TOP):
        expert = pos_ref[0:rows, TOP + k : TOP + k + 1].astype(jnp.int32)
        picked = jnp.sum(jnp.where(lane == expert, logits, 0.0), axis=1, keepdims=True)
        scores.append(jax.nn.sigmoid(picked))
    total = functools.reduce(lambda a, b: a + b, scores)
    out = jnp.zeros((rows, EXPERTS), F32)
    for k in range(TOP):
        out = jnp.where(lane == k, scores[k] / total, out)
    out_ref[...] = out


def combine_kernel(pos_ref, weight_ref, res_ref, context_ref, *refs, sub_local, width):
    blocks, (out_hbm_ref, out_ref, sem) = refs[:-3], refs[-3:]
    tokens = res_ref.shape[0]
    rows = sub_local * tokens
    returned = jnp.concatenate([ref[...] for ref in blocks], axis=0)
    slots = returned.shape[0]
    lane = lax.broadcasted_iota(jnp.int32, (rows, slots), 1)
    moe = jnp.zeros((rows, width), F32)
    for k in range(TOP):
        flat = pos_ref[0:rows, k : k + 1].astype(jnp.int32)
        hot = (lane == flat).astype(F32).astype(BF16)
        picked = jnp.dot(hot, returned, preferred_element_type=F32)
        moe = moe + weight_ref[:, k : k + 1] * picked
    stores = []
    for s in range(sub_local):
        at = slice(s * width, (s + 1) * width)
        total = res_ref[:, at].astype(F32) + context_ref[:, at]
        out_ref[:, at] = (total + moe[s * tokens : (s + 1) * tokens]).astype(BF16)
        stores.append(pltpu.make_async_copy(out_ref.at[:, at], out_hbm_ref.at[:, at], sem.at[s]))
        stores[-1].start()
    for store in stores:
        store.wait()


def attend_kernel(
    length_ref,
    query_ref,
    key_ref,
    value_ref,
    cache_key_ref,
    cache_value_ref,
    normed_ref,
    router_ref,
    pos_ref,
    attention_ref,
    context_ref,
    gate_ref,
    spread_ref,
    gather_ref,
    new_key_ref,
    new_value_ref,
    rounded_ref,
    store_sem,
):
    tokens = query_ref.shape[0]
    unroll = math.gcd(tokens, 32)
    groups = key_ref.shape[1] // HD
    per_group = HEADS // KV_HEADS
    heads = groups * per_group
    pad = spread_ref.shape[0] // tokens
    cache_len = cache_key_ref.shape[1]
    scale = 1.0 / math.sqrt(HD)
    new_key_ref[...] = key_ref[...].astype(F32)
    new_value_ref[...] = value_ref[...].astype(F32)
    for h in range(heads, pad):
        spread_ref[pl.ds(h, tokens, stride=pad), :] = jnp.zeros((tokens, HD), F32)
    for h in range(heads):
        spread_ref[pl.ds(h, tokens, stride=pad), :] = query_ref[:, h * HD : (h + 1) * HD].astype(F32)
    lane = lax.broadcasted_iota(jnp.int32, (pad, cache_len), 1)
    row = lax.broadcasted_iota(jnp.int32, (pad, HD), 0)
    lane = lax.broadcasted_iota(jnp.int32, (pad, cache_len), 1)
    member = [(row >= g * per_group) & (row < (g + 1) * per_group) for g in range(groups)]

    def by_group(x):
        out = jnp.broadcast_to(x[:, 0:HD], (pad, HD))
        for g in range(1, groups):
            out = jnp.where(member[g], x[:, g * HD : (g + 1) * HD], out)
        return out

    for i in range(tokens // unroll):
        at = slice(i * unroll * pad, (i + 1) * unroll * pad)
        inner = [i * unroll + u for u in range(unroll)]
        queries = spread_ref[at, :]
        scores = []
        for u, t in enumerate(inner):
            own = queries[u * pad : (u + 1) * pad]
            query = jnp.concatenate([jnp.where(one, own, 0.0) for one in member], axis=1)
            scores.append(
                lax.dot_general(
                    query.astype(BF16),
                    cache_key_ref[t],
                    (((1,), (1,)), ((), ())),
                    preferred_element_type=F32,
                )
            )
        usable = jnp.concatenate([lane < length_ref[t] for t in inner], axis=0)
        scores = jnp.where(usable, jnp.concatenate(scores, axis=0) * scale, -1e30)
        new_key = jnp.concatenate([by_group(new_key_ref[t : t + 1, :]) for t in inner], axis=0)
        new_value = jnp.concatenate([by_group(new_value_ref[t : t + 1, :]) for t in inner], axis=0)
        fresh = jnp.sum(queries * new_key, axis=1, keepdims=True) * scale
        row_max = jnp.maximum(jnp.max(scores, axis=1, keepdims=True), fresh)
        expo = jnp.where(usable, jnp.exp(scores - row_max), 0.0)
        expo_new = jnp.exp(fresh - row_max)
        total = jnp.sum(expo, axis=1, keepdims=True) + expo_new
        probs = expo / total
        prob_new = (expo_new / total).astype(BF16).astype(F32)
        context = [
            by_group(
                jnp.dot(
                    probs[u * pad : (u + 1) * pad].astype(BF16),
                    cache_value_ref[t],
                    preferred_element_type=F32,
                )
            )
            for u, t in enumerate(inner)
        ]
        gather_ref[at, :] = jnp.concatenate(context, axis=0) + prob_new * new_value
    for h in range(heads):
        context = gather_ref[pl.ds(h, tokens, stride=pad), :]
        context_ref[:, h * HD : (h + 1) * HD] = context
        rounded_ref[:, h * HD : (h + 1) * HD] = context.astype(BF16)
    store = pltpu.make_async_copy(rounded_ref, attention_ref, store_sem)
    store.start()
    gate(normed_ref[...], router_ref[...], pos_ref, gate_ref)
    store.wait()


def ffn_kernel(*refs, n_block, per_owner):
    blocks = refs[:n_block]
    first_ref, second_ref, mine_ref, other_ref, rows_ref, out_ref = refs[n_block:]
    slots, width = blocks[0].shape
    lanes = range(width // HD)
    for b in range(n_block):
        block = blocks[b][...].astype(F32)
        for c in lanes:
            rows_ref[c, b * slots : (b + 1) * slots, :] = block[:, c * HD : (c + 1) * HD]
    depth = n_block * slots // per_owner
    at = [pl.ds(e, depth, stride=per_owner) for e in range(per_owner)]
    taken = [
        jnp.concatenate([rows_ref[c, a, :] for c in lanes], axis=1).astype(BF16) for a in at
    ]
    hidden = [
        jnp.dot(x, first_ref[e], preferred_element_type=F32) for e, x in enumerate(taken)
    ]
    hidden = [jax.nn.gelu(h).astype(BF16) for h in hidden]
    for e, h in enumerate(hidden):
        result = jnp.dot(h, second_ref[e], preferred_element_type=F32)
        for c in lanes:
            out_ref[c, at[e], :] = result[:, c * HD : (c + 1) * HD]
    split = n_block // 2 * slots
    for c in lanes:
        mine_ref[:, c * HD : (c + 1) * HD] = out_ref[c, 0:split, :]
        other_ref[:, c * HD : (c + 1) * HD] = out_ref[c, split : 2 * split, :].astype(BF16)


def reduce_kernel(mine_ref, other_ref, *out_refs):
    slots = out_refs[0].shape[0]
    for j, ref in enumerate(out_refs):
        at = slice(j * slots, (j + 1) * slots)
        ref[...] = (mine_ref[at, :] + other_ref[at, :].astype(F32)).astype(BF16)


def per_device(
    residual,
    norm_gain,
    router_weight,
    expert_ids,
    expert_in,
    expert_out,
    queries,
    new_keys,
    new_values,
    cache_keys,
    cache_values,
    lengths,
):
    width = D // SUB
    tokens = residual.shape[0]
    sub_local = residual.shape[1] // width
    n_owner = lax.axis_size("expert")
    n_mp = lax.axis_size("mp")
    assert n_mp == 2
    per_owner = expert_in.shape[0]
    slots = CAP * per_owner
    half = n_owner // 2
    rows = tokens * SUB
    gain = norm_gain.reshape(-1, HD)

    swap = [(0, 1), (1, 0)]
    order = [half // 2] + [j for j in range(1, half) if j != half // 2] + [0]
    ring = list(range(0, half, 2)) + list(range(1, half, 2))[::-1]

    def partners(j, back=False):
        pairs = []
        for e in range(n_owner):
            far = ring[(ring.index(e >> 1) + j) % half]
            for m in range(n_mp):
                pair = (e * n_mp + m, (2 * far + ((e ^ m) & 1)) * n_mp + m)
                pairs.append(pair[::-1] if back else pair)
        return pairs

    peer_residual = lax.ppermute(residual, "mp", swap)
    peer_gain = lax.ppermute(gain, "mp", swap)
    pos, sel, normed = in_vmem(
        functools.partial(route_kernel, sub_local=sub_local, per_owner=per_owner, n_owner=n_owner),
        (
            jax.ShapeDtypeStruct((rows, EXPERTS), F32),
            jax.ShapeDtypeStruct((half * slots, rows), BF16),
            jax.ShapeDtypeStruct((sub_local * tokens, width), BF16),
        ),
        hbm=(0, 1, 2),
        scratch_shapes=(
            pltpu.VMEM((SUB, TOP, tokens), jnp.int32),
            pltpu.VMEM(residual.shape, BF16),
            pltpu.VMEM(gain.shape, BF16),
            pltpu.SemaphoreType.DMA((3,)),
        ),
        cost=20.0,
        name="route",
    )(expert_ids.transpose(1, 2, 0), residual, gain)
    sent = in_vmem(
        functools.partial(dispatch_kernel, sub_local=sub_local, width=width),
        tuple(jax.ShapeDtypeStruct((slots, width), BF16) for _ in range(half)),
        cost=20.0,
        name="dispatch",
    )(normed, peer_residual, peer_gain, sel)

    own = [None] * half
    for j in order:
        own[j] = lax.ppermute(sent[j], ("expert", "mp"), partners(j))
    groups = new_keys.shape[1] // HD
    pad = -(-groups * (HEADS // KV_HEADS) // 8) * 8
    attention, context, weights = in_vmem(
        attend_kernel,
        (
            jax.ShapeDtypeStruct(queries.shape, BF16),
            jax.ShapeDtypeStruct(queries.shape, F32),
            jax.ShapeDtypeStruct((sub_local * tokens, EXPERTS), F32),
        ),
        smem=(0,),
        hbm_out=(0,),
        scratch_shapes=(
            pltpu.VMEM((tokens * pad, HD), F32),
            pltpu.VMEM((tokens * pad, HD), F32),
            pltpu.VMEM(new_keys.shape, F32),
            pltpu.VMEM(new_values.shape, F32),
            pltpu.VMEM(queries.shape, BF16),
            pltpu.SemaphoreType.DMA,
        ),
        cost=4.0,
        name="attend",
    )(
        lengths,
        queries,
        new_keys,
        new_values,
        cache_keys,
        cache_values,
        normed,
        router_weight,
        pos,
    )
    peer = [None] * half
    for j in order:
        peer[j] = lax.ppermute(own[j], "mp", swap)

    def expert_pass(chosen, name):
        mine, other = in_vmem(
            functools.partial(ffn_kernel, n_block=2 * len(chosen), per_owner=per_owner),
            (
                jax.ShapeDtypeStruct((len(chosen) * slots, width), F32),
                jax.ShapeDtypeStruct((len(chosen) * slots, width), BF16),
            ),
            scratch_shapes=(
                pltpu.VMEM((width // HD, 2 * len(chosen) * slots, HD), F32),
                pltpu.VMEM((width // HD, 2 * len(chosen) * slots, HD), F32),
            ),
            room=12 << 20,
            cost=5.0,
            name=name,
        )(*[own[j] for j in chosen], *[peer[j] for j in chosen], expert_in, expert_out)
        return in_vmem(
            reduce_kernel,
            tuple(jax.ShapeDtypeStruct((slots, width), BF16) for _ in chosen),
            name="reduce",
        )(mine, lax.ppermute(other, "mp", swap))

    back = [None] * half
    for j, block in zip(order, expert_pass(order, "ffn")):
        back[j] = lax.ppermute(block, ("expert", "mp"), partners(j, back=True))
    peer_back = [None] * half
    for j in order:
        peer_back[j] = lax.ppermute(back[j], "mp", swap)
    (mixed,) = in_vmem(
        functools.partial(combine_kernel, sub_local=sub_local, width=width),
        (jax.ShapeDtypeStruct(residual.shape, BF16),),
        hbm_out=(0,),
        scratch_shapes=(
            pltpu.VMEM(residual.shape, BF16),
            pltpu.SemaphoreType.DMA((sub_local,)),
        ),
        name="combine",
    )(pos, weights, residual, context, *back, *peer_back)
    return (attention, mixed)


def solution(mesh):
    placed = (
        P(("groups", "expert"), "mp"),
        P("mp"),
        P(),
        P(("groups", "expert"), None, None),
        P("expert", None, "mp"),
        P("expert", "mp", None),
        P(("groups", "expert"), "mp"),
        P(("groups", "expert"), "mp"),
        P(("groups", "expert"), "mp"),
        P(("groups", "expert"), None, "mp"),
        P(("groups", "expert"), None, "mp"),
        P(("groups", "expert")),
    )
    return jax.shard_map(
        per_device,
        mesh=mesh,
        in_specs=placed,
        out_specs=(P(("groups", "expert"), "mp"), P(("groups", "expert"), "mp")),
        check_vma=False,
    )
```
